32 devices in a mesh: dp: 8 (over z, x), seq: 4 (over y, core).
Axes of the slice: x: 2, y: 2, z: 4, core: 2. Of those that a mesh axis runs over, the one named last changes fastest.
Arguments:
- tokens: bfloat16 [16, 1536, 768], P('dp', 'seq'), may hold values from -6 to 6
- cube_lengths: int32 [16], P('dp'), may hold values from 864 to 1536, as said below
- key_mask: int32 [16, 1536], P('dp'), may hold values from 0 to 1, as said below
- cotangent: bfloat16 [16, 1536, 768], P('dp', 'seq'), may hold values from -6 to 6
- norm_gain: bfloat16 [768], P(('dp', 'seq')), may hold values from 0.099609375 to 1.8984375
- norm_shift: bfloat16 [768], P(('dp', 'seq')), may hold values from -3 to 3
- proj_weight: bfloat16 [768, 2304], P(('dp', 'seq')), may hold values from -0.21875 to 0.21875
- query_bias: bfloat16 [768], P(('dp', 'seq')), may hold values from -3 to 3
- value_bias: bfloat16 [768], P(('dp', 'seq')), may hold values from -0.29882812 to 0.29882812
- merge_weight: bfloat16 [768, 768], P(('dp', 'seq')), may hold values from -4 to 4
- merge_bias: bfloat16 [768], P(('dp', 'seq')), may hold values from -2 to 2
- mlp_gain: bfloat16 [768], P(('dp', 'seq')), may hold values from 0.099609375 to 1.8984375
- mlp_shift: bfloat16 [768], P(('dp', 'seq')), may hold values from -3 to 3
- expand_weight: bfloat16 [768, 3072], P(('dp', 'seq')), may hold values from -0.21875 to 0.21875
- expand_bias: bfloat16 [3072], P(('dp', 'seq')), may hold values from -3 to 3
- reduce_weight: bfloat16 [3072, 768], P(('dp', 'seq')), may hold values from -0.109375 to 0.109375
- reduce_bias: bfloat16 [768], P(('dp', 'seq')), may hold values from -2 to 2
Outputs:
- activations: bfloat16 [16, 1536, 768], P('dp', 'seq')
- input_grad: float32 [16, 1536, 768], P('dp', 'seq')
- norm_gain_grad: float32 [768], P(('dp', 'seq'))
- norm_shift_grad: float32 [768], P(('dp', 'seq'))
- proj_weight_grad: float32 [768, 2304], P(('dp', 'seq'))
- query_bias_grad: float32 [768], P(('dp', 'seq'))
- value_bias_grad: float32 [768], P(('dp', 'seq'))
- merge_weight_grad: float32 [768, 768], P(('dp', 'seq'))
- merge_bias_grad: float32 [768], P(('dp', 'seq'))
- mlp_gain_grad: float32 [768], P(('dp', 'seq'))
- mlp_shift_grad: float32 [768], P(('dp', 'seq'))
- expand_weight_grad: float32 [768, 3072], P(('dp', 'seq'))
- expand_bias_grad: float32 [3072], P(('dp', 'seq'))
- reduce_weight_grad: float32 [3072, 768], P(('dp', 'seq'))
- reduce_bias_grad: float32 [768], P(('dp', 'seq'))
The draws below stay inside these ranges and needn't reach their ends.
Inputs may be any that keep to these rules, and one draw needn't show every extreme that they name: `cube_lengths`: each cube holds 1536 or 864 tokens and its remaining slots are padding; cube 0 holds 1536 and cube 1 holds 864. `key_mask`: slot 0 of every cube is 1.
All inputs are finite; a program needn't handle non-finite values.
Results may differ from the reference program's by a relative error of at most 0.012.
Values may be sent and summed in bfloat16 or wider, within the bound.
A program may use at most 192 MiB of HBM per device.

```python
import jax
import jax.numpy as jnp
from jax import lax

D = 768
H = 12
HD = 64
FF = 3072
L = 1536
SHORT = 864
CUBES = 16


def draw_cube_lengths(key, part):
    pick = jax.random.randint(key, (CUBES,), 0, 2)
    lengths = jnp.where(pick > 0, L, SHORT)
    index = jnp.arange(CUBES)
    lengths = jnp.where(index == 0, L, jnp.where(index == 1, SHORT, lengths))
    return lengths.astype(jnp.int32)


def draw_key_mask(key, part):
    picks = jax.random.randint(key, (CUBES, L), 0, 4)
    masked = (picks > 0).astype(jnp.int32)
    leading = (jnp.arange(L) == 0)[None, :]
    return jnp.where(leading, 1, masked).astype(jnp.int32)


def level_of(rng, shape, pieces, smallest, top_value):
    def one(dim, shards_of):
        heights = jax.random.uniform(jax.random.fold_in(jax.random.fold_in(rng, 6), dim), (shards_of,), jnp.float32, smallest / len(pieces), top_value / len(pieces))
        return jnp.repeat(jnp.exp(heights), shape[dim] // shards_of).reshape((-1,) + (1,) * (len(shape) - dim - 1))

    level = one(*pieces[0])
    for cut in pieces[1:]:
        level = level * one(*cut)
    return level


def scatter_about(rng, dims, scale, bound, shards=(), kind=jnp.bfloat16):
    level = level_of(rng, dims, shards, -0.22, 0.18) if shards else 1.0
    entries = jax.random.normal(rng, dims, jnp.float32) * scale * level
    return jnp.minimum(jnp.maximum(entries, -bound), bound).astype(kind)


def setup_inputs(seed: int = 0) -> dict:
    streams_of = jax.random.split(jax.random.key(seed), 18)
    tokens = scatter_about(streams_of[0], (CUBES, L, D), 1.0, 6.0, ((0, 8), (1, 4)))
    cube_lengths = draw_cube_lengths(jax.random.fold_in(streams_of[17], 71), 0)
    key_mask = draw_key_mask(jax.random.fold_in(streams_of[17], 71), 0)
    cotangent = scatter_about(streams_of[3], (CUBES, L, D), 1.0, 6.0, ((0, 8), (1, 4)))
    norm_gain = jnp.clip(1.0 + 0.18 * jax.random.normal(streams_of[4], (D,), jnp.float32), 0.099609375, 1.8984375).astype(jnp.bfloat16)
    norm_shift = scatter_about(streams_of[5], (D,), 0.5, 3.0, ((0, 32),))
    proj_weight = scatter_about(streams_of[6], (D, 3 * D), D ** -0.5, 0.21875, ((0, 32),))
    query_bias = scatter_about(streams_of[7], (D,), 0.5, 3.0, ((0, 32),))
    value_bias = scatter_about(streams_of[8], (D,), 0.05, 0.29882812, ((0, 32),))
    merge_weight = scatter_about(streams_of[9], (D, D), (D * 4 // L) ** -0.5, 4.0, ((0, 32),))
    merge_bias = scatter_about(streams_of[10], (D,), 0.3, 2.0, ((0, 32),))
    mlp_gain = jnp.clip(1.0 + 0.18 * jax.random.normal(streams_of[11], (D,), jnp.float32), 0.099609375, 1.8984375).astype(jnp.bfloat16)
    mlp_shift = scatter_about(streams_of[12], (D,), 0.5, 3.0, ((0, 32),))
    expand_weight = scatter_about(streams_of[13], (D, FF), D ** -0.5, 0.21875, ((0, 32),))
    expand_bias = scatter_about(streams_of[14], (FF,), 0.5, 3.0, ((0, 32),))
    reduce_weight = scatter_about(streams_of[15], (FF, D), FF ** -0.5, 0.109375, ((0, 32),))
    reduce_bias = scatter_about(streams_of[16], (D,), 0.3, 2.0, ((0, 32),))
    return {"tokens": tokens, "cube_lengths": cube_lengths, "key_mask": key_mask, "cotangent": cotangent, "norm_gain": norm_gain, "norm_shift": norm_shift, "proj_weight": proj_weight, "query_bias": query_bias, "value_bias": value_bias, "merge_weight": merge_weight, "merge_bias": merge_bias, "mlp_gain": mlp_gain, "mlp_shift": mlp_shift, "expand_weight": expand_weight, "expand_bias": expand_bias, "reduce_weight": reduce_weight, "reduce_bias": reduce_bias}


@jax.custom_vjp
def low(v):
    return lax.optimization_barrier(v.astype(jnp.bfloat16)).astype(jnp.float32)

@jax.custom_vjp
def low_back(v):
    return v

def low_keep(v):
    return (low(v), None)

def low_pass(kept, grad):
    return (grad,)

def back_keep(v):
    return (v, None)

def back_low(kept, grad):
    return (low(grad),)
low.defvjp(low_keep, low_pass)
low_back.defvjp(back_keep, back_low)
EPSILON = 1e-06

def norm_rows(v, gain, shift):
    mean = lax.optimization_barrier(jnp.mean(v, axis=-1, keepdims=True))
    center = v - mean
    spread = lax.optimization_barrier(jnp.mean(center * center, axis=-1, keepdims=True))
    return center * lax.rsqrt(spread + EPSILON) * gain + shift

def matmul(left, right):
    return jnp.dot(left, right, precision=lax.Precision.HIGHEST)

def split_heads(t):
    return t.reshape(t.shape[0], H, HD).transpose(1, 0, 2)

def block(x, valid, params):
    norm_gain, norm_shift, proj_weight, query_bias, value_bias, merge_weight, merge_bias, mlp_gain, mlp_shift, expand_weight, expand_bias, reduce_weight, reduce_bias = params
    width = x.shape[1]
    first = low(norm_rows(x, norm_gain, norm_shift))
    packed = matmul(first, proj_weight)
    query = low(low_back(packed[:, :width] + query_bias))
    keys = low(low_back(packed[:, width:2 * width]))
    values = low(low_back(packed[:, 2 * width:] + value_bias))
    scores = low_back(jnp.einsum('hqd,hkd->hqk', split_heads(query), split_heads(keys), precision=lax.Precision.HIGHEST)) * HD ** (-0.5)
    scores = jnp.where(valid[None, None, :] > 0, scores, -1e+30)
    top = lax.optimization_barrier(jnp.max(scores, axis=-1, keepdims=True))
    expo = jnp.exp(scores - top)
    probs = low(expo / lax.optimization_barrier(jnp.sum(expo, axis=-1, keepdims=True)))
    heads_out = jnp.einsum('hqk,hkd->hqd', probs, split_heads(values), precision=lax.Precision.HIGHEST)
    attn = low(low_back(heads_out.transpose(1, 0, 2).reshape(x.shape[0], width)))
    merged = low_back(matmul(attn, merge_weight) + merge_bias)
    middle = x + merged
    second = low(norm_rows(middle, mlp_gain, mlp_shift))
    hidden = low_back(matmul(second, expand_weight) + expand_bias)
    act = low(jax.nn.gelu(hidden, approximate=False))
    output = low_back(matmul(act, reduce_weight) + reduce_bias)
    return middle + output

def reference(tokens, cube_lengths, key_mask, cotangent, norm_gain, norm_shift, proj_weight, query_bias, value_bias, merge_weight, merge_bias, mlp_gain, mlp_shift, expand_weight, expand_bias, reduce_weight, reduce_bias):
    params = tuple((p.astype(jnp.float32) for p in (norm_gain, norm_shift, proj_weight, query_bias, value_bias, merge_weight, merge_bias, mlp_gain, mlp_shift, expand_weight, expand_bias, reduce_weight, reduce_bias)))
    positions = jnp.arange(L, dtype=jnp.int32)
    valid = ((key_mask > 0) & (positions[None, :] < cube_lengths[:, None])).astype(jnp.float32)

    def per_cube(totals, item):
        inputs, upstream, usable = item

        def layer(values_in, weights):
            return block(values_in, usable, weights)
        result, pull = jax.vjp(layer, inputs, params)
        input_part, param_parts = pull(upstream)
        totals = jax.tree.map(jnp.add, totals, param_parts)
        return (totals, (result.astype(jnp.bfloat16), input_part))
    zeros = jax.tree.map(jnp.zeros_like, params)
    grads, (outputs, input_grad) = lax.scan(per_cube, zeros, (tokens.astype(jnp.float32), cotangent.astype(jnp.float32), valid))
    return (outputs, input_grad, grads[0], grads[1], grads[2], grads[3], grads[4], grads[5], grads[6], grads[7], grads[8], grads[9], grads[10], grads[11], grads[12])
```

```python
import functools

import jax
import jax.numpy as jnp
from jax import lax
from jax.experimental import pallas as pl
from jax.experimental.pallas import tpu as pltpu
from jax.sharding import PartitionSpec as P

HD = 64
LANES = 128
EPSILON = 1e-06
F32 = jnp.float32
BF16 = jnp.bfloat16
ALL = ("dp", "seq")


def head_lanes(rows, h):
    lane = lax.broadcasted_iota(jnp.int32, (rows, 128), 1)
    return (lane < 64) if h == 0 else (lane >= 64)

def fwd_kernel(tq, q_ref, k_ref, v_ref, bias_ref, o_ref, lse_ref):
    k = k_ref[...]
    v = v_ref[...]
    bias = bias_ref[...]
    def body(i, _):
        rows = pl.ds(pl.multiple_of(i * tq, tq), tq)
        q = q_ref[rows, :]
        outs = []
        for h in range(2):
            keep = head_lanes(tq, h)
            qh = jnp.where(keep, q, jnp.zeros_like(q))
            s = lax.dot_general(qh, k, (((1,), (1,)), ((), ())), preferred_element_type=F32) + bias
            top = jnp.max(s, axis=1, keepdims=True)
            e = jnp.exp(s - top)
            total = jnp.sum(e, axis=1, keepdims=True)
            o = jnp.dot(e.astype(BF16), v, preferred_element_type=F32) / total
            lse = top + jnp.log(total)
            lse_ref[0, h:h + 1, rows] = jnp.broadcast_to(lse, (tq, 128)).T[0:1, :]
            outs.append(o)
        o_ref[rows, :] = jnp.where(head_lanes(tq, 0), outs[0], outs[1]).astype(BF16)
        return 0
    lax.fori_loop(0, q_ref.shape[0] // tq, body, 0)

def attn_fwd(q, k, v, bias, tq=256):
    R, D = q.shape; K = k.shape[0]; P = D // 128
    return pl.pallas_call(
        functools.partial(fwd_kernel, tq),
        grid=(P,),
        in_specs=[pl.BlockSpec((R,128), lambda p:(0,p)), pl.BlockSpec((K,128), lambda p:(0,p)), pl.BlockSpec((K,128), lambda p:(0,p)), pl.BlockSpec((1,K), lambda p:(0,0))],
        out_specs=[pl.BlockSpec((R,128), lambda p:(0,p)), pl.BlockSpec((1,2,R), lambda p:(p,0,0))],
        out_shape=[jax.ShapeDtypeStruct((R,D),BF16), jax.ShapeDtypeStruct((P,2,R),F32)],
        compiler_params=pltpu.CompilerParams(vmem_limit_bytes=60<<20),
        name="attn_fwd",
    )(q,k,v,bias)

def bwd_kernel(tq, q_ref, k_ref, v_ref, g_ref, o_ref, lse_ref, bias_ref, dq_ref, dk_ref, dv_ref, dk_acc, dv_acc):
    k = k_ref[...]
    v = v_ref[...]
    K = k.shape[0]
    bias = bias_ref[...]
    dk_acc[...] = jnp.zeros_like(dk_acc)
    dv_acc[...] = jnp.zeros_like(dv_acc)
    def body(i, _):
        rows = pl.ds(pl.multiple_of(i * tq, tq), tq)
        q = q_ref[rows, :]
        g = g_ref[rows, :]
        go = g.astype(F32) * o_ref[rows, :].astype(F32)
        dq = None
        for h in range(2):
            keep = head_lanes(tq, h)
            qh = jnp.where(keep, q, jnp.zeros_like(q))
            gh = jnp.where(keep, g, jnp.zeros_like(g))
            delta = jnp.sum(jnp.where(keep, go, 0.0), axis=1, keepdims=True)
            delta = jnp.broadcast_to(delta, (tq, 128)).T[0:1, :]
            lse = lse_ref[0, h:h + 1, rows]
            s = lax.dot_general(k, qh, (((1,), (1,)), ((), ())), preferred_element_type=F32)
            p = jnp.exp(s + bias - lse)
            dp = lax.dot_general(v, gh, (((1,), (1,)), ((), ())), preferred_element_type=F32)
            ds = (p * (dp - delta)).astype(BF16)
            dv_acc[...] += jnp.dot(p.astype(BF16), gh, preferred_element_type=F32)
            dk_acc[...] += jnp.dot(ds, qh, preferred_element_type=F32)
            kh = jnp.where(head_lanes(K, h), k, jnp.zeros_like(k))
            part = lax.dot_general(ds, kh, (((0,), (0,)), ((), ())), preferred_element_type=F32)
            dq = part if dq is None else dq + part
        dq_ref[rows, :] = (dq * 0.125).astype(BF16)
        return 0
    lax.fori_loop(0, q_ref.shape[0] // tq, body, 0)
    dk_ref[...] = dk_acc[...].astype(BF16)
    dv_ref[...] = dv_acc[...].astype(BF16)

def attn_bwd(q, k, v, g, o, lse, bias_col, tq=256):
    R, D = q.shape; K = k.shape[0]; P = D // 128
    rs = pl.BlockSpec((R,128), lambda p:(0,p)); ks = pl.BlockSpec((K,128), lambda p:(0,p))
    return pl.pallas_call(
        functools.partial(bwd_kernel, tq),
        grid=(P,),
        in_specs=[rs, ks, ks, rs, rs, pl.BlockSpec((1,2,R), lambda p:(p,0,0)), pl.BlockSpec((K,1), lambda p:(0,0))],
        out_specs=[rs, ks, ks],
        out_shape=[jax.ShapeDtypeStruct((R,D),BF16), jax.ShapeDtypeStruct((K,D),BF16), jax.ShapeDtypeStruct((K,D),BF16)],
        scratch_shapes=[pltpu.VMEM((K,128),F32), pltpu.VMEM((K,128),F32)],
        compiler_params=pltpu.CompilerParams(vmem_limit_bytes=60<<20),
        name="attn_bwd",
    )(q,k,v,g,o,lse,bias_col)


def norm_rows(v, gain, shift):
    mean = jnp.mean(v, axis=-1, keepdims=True)
    center = v - mean
    spread = jnp.mean(center * center, axis=-1, keepdims=True)
    return center * lax.rsqrt(spread + EPSILON) * gain + shift


def gelu_exact(v):
    return jax.nn.gelu(v, approximate=False)


def shards(
    tokens,
    cube_lengths,
    key_mask,
    cotangent,
    norm_gain,
    norm_shift,
    proj_weight,
    query_bias,
    value_bias,
    merge_weight,
    merge_bias,
    mlp_gain,
    mlp_shift,
    expand_weight,
    expand_bias,
    reduce_weight,
    reduce_bias,
):
    slots, local_len, width = tokens.shape
    full_len = key_mask.shape[1]
    seq = full_len // local_len
    half = seq // slots
    rows = slots * local_len
    me = lax.axis_index("seq")
    cube = me // half

    across = [(i, (i + half) % seq) for i in range(seq)]
    around = [
        [(g * half + i, g * half + (i + r) % half) for g in range(slots) for i in range(half)]
        for r in range(half)
    ]

    def swap(pair):
        own = lax.dynamic_index_in_dim(pair, cube, 0, keepdims=False)
        other = lax.dynamic_index_in_dim(pair, 1 - cube, 0, keepdims=False)
        return own, lax.ppermute(other, "seq", across)

    def swap_back(own, other):
        back = lax.ppermute(other, "seq", across).astype(own.dtype)
        first = jnp.where(cube == 0, own, back)
        second = jnp.where(cube == 0, back, own)
        return jnp.stack([first, second])

    def gather(shard):
        return lax.all_gather(shard, ALL, axis=0, tiled=True)

    vectors = (
        norm_gain,
        norm_shift,
        query_bias,
        value_bias,
        merge_bias,
        mlp_gain,
        mlp_shift,
        reduce_bias,
        expand_bias,
    )
    packed_vectors = lax.all_gather(jnp.concatenate(vectors), ALL, axis=0)
    wide = []
    start = 0
    for vector in vectors:
        size = vector.shape[0]
        wide.append(packed_vectors[:, start : start + size].reshape(-1).astype(F32))
        start += size
    (
        gain_first,
        shift_first,
        query_add,
        value_add,
        merge_add,
        gain_second,
        shift_second,
        reduce_add,
        expand_add,
    ) = wide
    proj_full = gather(proj_weight)
    own_tokens, other_tokens = swap(tokens)
    own_cot, other_cot = swap(cotangent)
    resid = jnp.concatenate([own_tokens, other_tokens]).astype(F32)
    upstream = jnp.concatenate([own_cot, other_cot])
    merge_full = gather(merge_weight)
    expand_full = gather(expand_weight)
    reduce_full = gather(reduce_weight)

    length = lax.dynamic_index_in_dim(cube_lengths, cube, 0, keepdims=False)
    mask = lax.dynamic_index_in_dim(key_mask, cube, 0, keepdims=False)
    bias_all = jnp.where((mask > 0) & (jnp.arange(full_len) < length), 0.0, -1e30).astype(F32)
    blocks = []
    for r in range(half):
        device = cube * half + (me + half - r) % half
        for index in (device, (device + half) % seq):
            blocks.append(lax.dynamic_slice_in_dim(bias_all, index * local_len, local_len))
    bias = jnp.concatenate(blocks)

    first_f, first_pull = jax.vjp(norm_rows, resid, gain_first, shift_first)
    first = first_f.astype(BF16)
    packed = jnp.dot(first, proj_full, preferred_element_type=F32)
    query = (packed[:, :width] + query_add).astype(BF16)
    query = query * jnp.asarray(HD**-0.5, BF16)
    keys = packed[:, width : 2 * width].astype(BF16)
    values = (packed[:, 2 * width :] + value_add).astype(BF16)
    keys_all = jnp.concatenate([keys] + [lax.ppermute(keys, "seq", a) for a in around[1:]])
    values_all = jnp.concatenate([values] + [lax.ppermute(values, "seq", a) for a in around[1:]])
    attn, lse = attn_fwd(query, keys_all, values_all, bias[None, :])

    middle = resid + jnp.dot(attn, merge_full, preferred_element_type=F32) + merge_add
    second_f, second_pull = jax.vjp(norm_rows, middle, gain_second, shift_second)
    second = second_f.astype(BF16)
    hidden = jnp.dot(second, expand_full, preferred_element_type=F32) + expand_add
    act_f, gelu_pull = jax.vjp(gelu_exact, hidden)
    act = act_f.astype(BF16)
    output = middle + jnp.dot(act, reduce_full, preferred_element_type=F32) + reduce_add
    output = output.astype(BF16)
    activations = swap_back(output[:local_len], output[local_len:])

    def scatter(grad):
        return lax.psum_scatter(
            grad.astype(BF16), ALL, scatter_dimension=0, tiled=True
        ).astype(F32)

    upstream_f = upstream.astype(F32)
    reduce_bias_grad = jnp.sum(upstream_f, axis=0)
    reduce_weight_grad = scatter(
        jnp.einsum("rf,rd->fd", act, upstream, preferred_element_type=F32)
    )
    act_grad = jnp.einsum("rd,fd->rf", upstream, reduce_full, preferred_element_type=F32)
    hidden_grad = gelu_pull(act_grad)[0].astype(BF16)
    expand_bias_grad = jnp.sum(hidden_grad.astype(F32), axis=0)
    expand_weight_grad = scatter(
        jnp.einsum("rd,rf->df", second, hidden_grad, preferred_element_type=F32)
    )
    second_grad = jnp.einsum("rf,df->rd", hidden_grad, expand_full, preferred_element_type=F32)
    middle_norm, mlp_gain_grad, mlp_shift_grad = second_pull(second_grad)
    middle_grad = upstream_f + middle_norm
    merged_grad = middle_grad.astype(BF16)
    merge_bias_grad = jnp.sum(merged_grad.astype(F32), axis=0)
    merge_weight_grad = scatter(
        jnp.einsum("rd,re->de", attn, merged_grad, preferred_element_type=F32)
    )
    attn_grad = jnp.einsum("re,de->rd", merged_grad, merge_full, preferred_element_type=F32)
    attn_grad = attn_grad.astype(BF16)

    query_grad, key_parts, value_parts = attn_bwd(
        query, keys_all, values_all, attn_grad, attn, lse, bias[:, None]
    )

    def collect(parts):
        total = parts[:rows].astype(F32)
        for r in range(1, half):
            sent = parts[r * rows : (r + 1) * rows]
            back = [(j, i) for i, j in around[r]]
            total = total + lax.ppermute(sent, "seq", back).astype(F32)
        return total.astype(BF16)

    key_grad = collect(key_parts)
    value_grad = collect(value_parts)
    query_bias_grad = jnp.sum(query_grad.astype(F32), axis=0)
    value_bias_grad = jnp.sum(value_grad.astype(F32), axis=0)
    packed_grad = jnp.concatenate([query_grad, key_grad, value_grad], axis=1)
    proj_weight_grad = scatter(
        jnp.einsum("rd,re->de", first, packed_grad, preferred_element_type=F32)
    )
    first_grad = jnp.einsum("re,de->rd", packed_grad, proj_full, preferred_element_type=F32)
    resid_norm, norm_gain_grad, norm_shift_grad = first_pull(first_grad)
    input_sum = middle_grad + resid_norm
    input_grad = swap_back(input_sum[:local_len], input_sum[local_len:].astype(BF16))

    vector_grads = (
        norm_gain_grad,
        norm_shift_grad,
        query_bias_grad,
        value_bias_grad,
        merge_bias_grad,
        mlp_gain_grad,
        mlp_shift_grad,
        reduce_bias_grad,
        expand_bias_grad,
    )
    count = packed_vectors.shape[0]
    summed = lax.psum_scatter(
        jnp.concatenate([g.reshape(count, -1) for g in vector_grads], axis=1).reshape(-1),
        ALL,
        scatter_dimension=0,
        tiled=True,
    )
    small = []
    start = 0
    for vector in vectors:
        size = vector.shape[0]
        small.append(summed[start : start + size])
        start += size
    (
        norm_gain_grad,
        norm_shift_grad,
        query_bias_grad,
        value_bias_grad,
        merge_bias_grad,
        mlp_gain_grad,
        mlp_shift_grad,
        reduce_bias_grad,
        expand_bias_grad,
    ) = small
    return (
        activations,
        input_grad,
        norm_gain_grad,
        norm_shift_grad,
        proj_weight_grad,
        query_bias_grad,
        value_bias_grad,
        merge_weight_grad,
        merge_bias_grad,
        mlp_gain_grad,
        mlp_shift_grad,
        expand_weight_grad,
        expand_bias_grad,
        reduce_weight_grad,
        reduce_bias_grad,
    )


def solution(mesh):
    whole, part = P(ALL, None), P(ALL)
    block = P("dp", "seq", None)
    in_specs = (
        block,
        P("dp"),
        P("dp", None),
        block,
        part,
        part,
        whole,
        part,
        part,
        whole,
        part,
        part,
        part,
        whole,
        part,
        whole,
        part,
    )
    out_specs = (
        block,
        block,
        part,
        part,
        whole,
        part,
        part,
        whole,
        part,
        part,
        part,
        whole,
        part,
        whole,
        part,
    )
    return jax.shard_map(shards, mesh=mesh, in_specs=in_specs, out_specs=out_specs, check_vma=False)
```

```python
import functools

import jax
import jax.numpy as jnp
from jax import lax
from jax.experimental import pallas as pl
from jax.experimental.pallas import tpu as pltpu
from jax.sharding import PartitionSpec as P

HD = 64
LANES = 128
EPSILON = 1e-06
F32 = jnp.float32
BF16 = jnp.bfloat16
ALL = ("dp", "seq")


def head_lanes(rows, h):
    lane = lax.broadcasted_iota(jnp.int32, (rows, 128), 1)
    return (lane < 64) if h == 0 else (lane >= 64)

def fwd_kernel(tq, q_ref, k_ref, v_ref, bias_ref, o_ref, lse_ref):
    k = k_ref[...]
    v = v_ref[...]
    bias = bias_ref[...]
    def body(i, _):
        rows = pl.ds(pl.multiple_of(i * tq, tq), tq)
        q = q_ref[rows, :]
        outs = []
        for h in range(2):
            keep = head_lanes(tq, h)
            qh = jnp.where(keep, q, jnp.zeros_like(q))
            s = lax.dot_general(qh, k, (((1,), (1,)), ((), ())), preferred_element_type=F32) + bias
            top = jnp.max(s, axis=1, keepdims=True)
            e = jnp.exp(s - top)
            total = jnp.sum(e, axis=1, keepdims=True)
            o = jnp.dot(e.astype(BF16), v, preferred_element_type=F32) / total
            lse = top + jnp.log(total)
            lse_ref[0, h:h + 1, rows] = jnp.broadcast_to(lse, (tq, 128)).T[0:1, :]
            outs.append(o)
        o_ref[rows, :] = jnp.where(head_lanes(tq, 0), outs[0], outs[1]).astype(BF16)
        return 0
    lax.fori_loop(0, q_ref.shape[0] // tq, body, 0)

def attn_fwd(q, k, v, bias, tq=256):
    R, D = q.shape; K = k.shape[0]; P = D // 128
    return pl.pallas_call(
        functools.partial(fwd_kernel, tq),
        grid=(P,),
        in_specs=[pl.BlockSpec((R,128), lambda p:(0,p)), pl.BlockSpec((K,128), lambda p:(0,p)), pl.BlockSpec((K,128), lambda p:(0,p)), pl.BlockSpec((1,K), lambda p:(0,0))],
        out_specs=[pl.BlockSpec((R,128), lambda p:(0,p)), pl.BlockSpec((1,2,R), lambda p:(p,0,0))],
        out_shape=[jax.ShapeDtypeStruct((R,D),BF16), jax.ShapeDtypeStruct((P,2,R),F32)],
        compiler_params=pltpu.CompilerParams(vmem_limit_bytes=60<<20),
        name="attn_fwd",
    )(q,k,v,bias)

def bwd_kernel(tq, q_ref, k_ref, v_ref, g_ref, o_ref, lse_ref, bias_ref, dq_ref, dk_ref, dv_ref, dk_acc, dv_acc):
    k = k_ref[...]
    v = v_ref[...]
    K = k.shape[0]
    bias = bias_ref[...]
    dk_acc[...] = jnp.zeros_like(dk_acc)
    dv_acc[...] = jnp.zeros_like(dv_acc)
    def body(i, _):
        rows = pl.ds(pl.multiple_of(i * tq, tq), tq)
        q = q_ref[rows, :]
        g = g_ref[rows, :]
        go = g.astype(F32) * o_ref[rows, :].astype(F32)
        dq = None
        for h in range(2):
            keep = head_lanes(tq, h)
            qh = jnp.where(keep, q, jnp.zeros_like(q))
            gh = jnp.where(keep, g, jnp.zeros_like(g))
            delta = jnp.sum(jnp.where(keep, go, 0.0), axis=1, keepdims=True)
            delta = jnp.broadcast_to(delta, (tq, 128)).T[0:1, :]
            lse = lse_ref[0, h:h + 1, rows]
            s = lax.dot_general(k, qh, (((1,), (1,)), ((), ())), preferred_element_type=F32)
            p = jnp.exp(s + bias - lse)
            dp = lax.dot_general(v, gh, (((1,), (1,)), ((), ())), preferred_element_type=F32)
            ds = (p * (dp - delta)).astype(BF16)
            dv_acc[...] += jnp.dot(p.astype(BF16), gh, preferred_element_type=F32)
            dk_acc[...] += jnp.dot(ds, qh, preferred_element_type=F32)
            kh = jnp.where(head_lanes(K, h), k, jnp.zeros_like(k))
            part = lax.dot_general(ds, kh, (((0,), (0,)), ((), ())), preferred_element_type=F32)
            dq = part if dq is None else dq + part
        dq_ref[rows, :] = (dq * 0.125).astype(BF16)
        return 0
    lax.fori_loop(0, q_ref.shape[0] // tq, body, 0)
    dk_ref[...] = dk_acc[...].astype(BF16)
    dv_ref[...] = dv_acc[...].astype(BF16)

def attn_bwd(q, k, v, g, o, lse, bias_col, tq=256):
    R, D = q.shape; K = k.shape[0]; P = D // 128
    rs = pl.BlockSpec((R,128), lambda p:(0,p)); ks = pl.BlockSpec((K,128), lambda p:(0,p))
    return pl.pallas_call(
        functools.partial(bwd_kernel, tq),
        grid=(P,),
        in_specs=[rs, ks, ks, rs, rs, pl.BlockSpec((1,2,R), lambda p:(p,0,0)), pl.BlockSpec((K,1), lambda p:(0,0))],
        out_specs=[rs, ks, ks],
        out_shape=[jax.ShapeDtypeStruct((R,D),BF16), jax.ShapeDtypeStruct((K,D),BF16), jax.ShapeDtypeStruct((K,D),BF16)],
        scratch_shapes=[pltpu.VMEM((K,128),F32), pltpu.VMEM((K,128),F32)],
        compiler_params=pltpu.CompilerParams(vmem_limit_bytes=60<<20),
        name="attn_bwd",
    )(q,k,v,g,o,lse,bias_col)


MESH = pl.DeviceIdType.MESH


class Copies:
    def __init__(self, send, recv):
        self.send, self.recv, self.made = send, recv, []

    def make(self, src, dst, to):
        i = len(self.made)
        z, x, y, c = to
        copy = pltpu.make_async_remote_copy(
            src_ref=src,
            dst_ref=dst,
            send_sem=self.send.at[i],
            recv_sem=self.recv.at[i],
            device_id=(z * 2 + x, y * 2 + c),
            device_id_type=MESH,
        )
        self.made.append(copy)
        return copy


def place():
    dp, seq = lax.axis_index("dp"), lax.axis_index("seq")
    return dp // 2, dp % 2, seq // 2, seq % 2


def ring(layers):
    z, x, y, c = place()
    others = [((z + r) % layers, x, y, c) for r in range(1, layers)]
    return (z, x, y, 1 - c), (z, 1 - x, y, c), (z, x, 1 - y, c), others


def greet(layers):
    sibling, across_x, across_y, others = ring(layers)
    peers = [sibling, across_x, across_y] + others
    barrier = pltpu.get_barrier_semaphore()
    for z, x, y, c in peers:
        pl.semaphore_signal(
            barrier, inc=1, device_id=(z * 2 + x, y * 2 + c), device_id_type=MESH
        )
    pl.semaphore_wait(barrier, len(peers))


def cut_of(columns):
    return columns // 2 if columns % 256 == 0 else columns


KINDS = 10


def gather_phases(layers, shards, outs, send, recv, local):
    z, x, y, c = place()
    sibling, across_x, across_y, _ = ring(layers)
    above, below = ((z + 1) % layers, x, y, c), ((z + layers - 1) % layers, x, y, c)
    count = range(len(shards))

    def index(z, x, y, c):
        return ((z * 2 + x) * 2 + y) * 2 + c

    def copy(src, dst, a, kind, zs, to, sent=None):
        i = (a * KINDS + kind) * layers + zs
        j = (a * KINDS + (kind if sent is None else sent)) * layers + zs
        z, x, y, c = to
        return pltpu.make_async_remote_copy(
            src_ref=src,
            dst_ref=dst,
            send_sem=send.at[j],
            recv_sem=recv.at[i],
            device_id=(z * 2 + x, y * 2 + c),
            device_id_type=MESH,
        )

    mine = [
        pltpu.make_async_copy(shards[a], outs[a].at[index(z, x, y, c)], local.at[a]) for a in count
    ]
    sources = [(0, 0)]
    for d in range(1, layers):
        sources += [(1, d), (-1, d)]

    def unit(source, a):
        way, d = source
        zs = (z + layers - way * d) % layers
        there = None if d == 0 else (z >= d if way == 1 else z + d < layers)
        out = outs[a]
        here = out.at[index(zs, x, y, c)]
        src = shards[a] if d == 0 else here
        px = out.at[index(zs, 1 - x, y, c)]
        py = out.at[index(zs, x, 1 - y, c)]
        pd = out.at[index(zs, 1 - x, 1 - y, c)]
        columns = shards[a].shape[-1]
        cut = cut_of(columns)
        left = px if cut == columns else px.at[:, pl.ds(0, cut)]
        relay = [copy(left, left, a, 7, zs, across_y)]
        if cut < columns:
            right = py.at[:, pl.ds(cut, cut)]
            relay.append(copy(right, right, a, 8, zs, across_x))
        up = copy(src, here, a, 0, zs, above)
        down = copy(src, here, a, 0, zs, below, 9 if d == 0 else None)
        spread = [
            copy(src, here, a, 1, zs, across_x),
            copy(src, here, a, 2, zs, across_y),
            copy(src, here, a, 3, zs, sibling),
        ]
        sib = [copy(p, p, a, 4 + i, zs, sibling) for i, p in enumerate((px, py, pd))]
        return there, up, down, spread, relay, sib

    units = {(s, a): unit(s, a) for s in sources for a in count}

    def when(there, body):
        if there is None:
            body()
        else:
            pl.when(there)(body)

    def onward(source, up, down, act):
        way, d = source
        if way >= 0 and d < layers - 1:
            pl.when(z + 1 < layers)(lambda: act(up))
        if way <= 0 and d < layers - 1:
            pl.when(z > 0)(lambda: act(down))

    def second(source):
        for a in count:
            there, up, down, spread, relay, sib = units[source, a]

            def body():
                if source[1]:
                    up.wait_recv()
                else:
                    mine[a].start()
                onward(source, up, down, lambda copy: copy.start())
                for copy in spread:
                    copy.start()

            when(there, body)

    def third(source):
        for a in count:
            there, up, down, spread, relay, sib = units[source, a]

            def body():
                spread[0].wait_recv()
                relay[0].start()
                sib[0].start()
                spread[1].wait_recv()
                for copy in relay[1:]:
                    copy.start()
                sib[1].start()

            when(there, body)

    def fourth(source):
        for a in count:
            there, up, down, spread, relay, sib = units[source, a]

            def body():
                for copy in relay:
                    copy.wait_recv()
                sib[2].start()

            when(there, body)

    def last(source):
        for a in count:
            there, up, down, spread, relay, sib = units[source, a]

            def body():
                for copy in [spread[2]] + sib:
                    copy.wait_recv()
                onward(source, up, down, lambda copy: copy.wait_send())
                for copy in spread + relay + sib:
                    copy.wait_send()
                if source[1] == 0:
                    mine[a].wait()

            when(there, body)

    phases = []
    for d in range(layers + 2):
        for way in (0,) if d == 0 else (1, -1):
            if d < layers:
                phases.append(functools.partial(second, (way, d)))
        for step, lag in ((third, 1), (fourth, 2)):
            for way in (0,) if d == lag else (1, -1):
                if lag <= d < layers + lag:
                    phases.append(functools.partial(step, (way, d - lag)))
    return phases + [functools.partial(last, s) for s in sources]


def gather_kernel(layers, count, *refs):
    shards, outs = refs[:count], refs[count : 2 * count]
    greet(layers)
    for phase in gather_phases(layers, shards, outs, *refs[2 * count :]):
        phase()


def gather_scratch(layers, count):
    return [
        pltpu.SemaphoreType.DMA((count * KINDS * layers,)),
        pltpu.SemaphoreType.DMA((count * KINDS * layers,)),
        pltpu.SemaphoreType.DMA((count,)),
    ]


def gather_all(layers, shards, ident, name):
    devices = layers * 8
    return pl.pallas_call(
        functools.partial(gather_kernel, layers, len(shards)),
        out_shape=[jax.ShapeDtypeStruct((devices,) + s.shape, s.dtype) for s in shards],
        in_specs=[pl.BlockSpec(memory_space=pltpu.VMEM)] * len(shards),
        out_specs=[pl.BlockSpec(memory_space=pl.ANY)] * len(shards),
        scratch_shapes=gather_scratch(layers, len(shards)),
        compiler_params=pltpu.CompilerParams(collective_id=ident, has_side_effects=True),
        name=name,
    )(*shards)


def scatter_scratch(layers, shapes, dtypes):
    made = []
    for (rows, columns), dtype in zip(shapes, dtypes):
        cut = cut_of(columns)
        made += [
            pltpu.VMEM((layers, 4, rows, columns), dtype),
            pltpu.VMEM((layers, 4, rows, columns), dtype),
            pltpu.VMEM((layers, rows, cut), dtype),
            pltpu.VMEM((layers, rows, cut), dtype),
            pltpu.VMEM((layers, rows, columns), dtype),
            pltpu.VMEM((layers, rows, columns), dtype),
            pltpu.VMEM((layers, rows, columns), dtype),
        ]
    return made


def scatter_count(layers, shapes):
    total = 0
    for _, columns in shapes:
        total += layers - 1 + layers * (4 if cut_of(columns) == columns else 5)
    return total


def scatter_phases(layers, grads, outs, scratch, send, recv, local):
    z, x, y, c = place()
    sibling, across_x, across_y, others = ring(layers)
    copies = Copies(send, recv)
    count = range(len(grads))
    kept, from_sib, diag, on_x, on_y, along, zs_of = {}, {}, {}, {}, {}, {}, {}
    order = list(range(1, layers)) + [0]
    for r in order:
        zs = (z + r) % layers
        zs_of[r] = zs
        for a in count:
            sums, terms, left, right, gx, gy, gz = scratch[7 * a : 7 * a + 7]
            columns = sums.shape[-1]
            cut = cut_of(columns)
            kept[r, a] = pltpu.make_async_copy(
                grads[a].at[zs, :, c], sums.at[zs], local.at[len(grads) * r + a]
            )
            from_sib[r, a] = copies.make(grads[a].at[zs, :, 1 - c], terms.at[zs], sibling)
            far = sums.at[zs, (1 - x) * 2 + 1 - y]
            if cut == columns:
                diag[r, a] = [copies.make(far, left.at[zs], across_y)]
            else:
                diag[r, a] = [
                    copies.make(far.at[:, pl.ds(0, cut)], left.at[zs], across_y),
                    copies.make(far.at[:, pl.ds(cut, cut)], right.at[zs], across_x),
                ]
            on_x[r, a] = copies.make(sums.at[zs, (1 - x) * 2 + y], gx.at[zs], across_x)
            on_y[r, a] = copies.make(sums.at[zs, x * 2 + 1 - y], gy.at[zs], across_y)
            if r:
                along[r, a] = copies.make(sums.at[zs, x * 2 + y], gz.at[r], others[r - 1])

    def first():
        for r in order:
            for a in count:
                kept[r, a].start()
                from_sib[r, a].start()

    def second(r, a):
        sums, terms = scratch[7 * a : 7 * a + 2]
        zs = zs_of[r]
        kept[r, a].wait()
        from_sib[r, a].wait_recv()
        for k in range(4):
            sums[zs, k] = sums[zs, k] + terms[zs, k]
        for copy in diag[r, a]:
            copy.start()

    def third(r, a):
        sums, _, left, right = scratch[7 * a : 7 * a + 4]
        zs = zs_of[r]
        cut = left.shape[-1]
        kx, ky = (1 - x) * 2 + y, x * 2 + 1 - y
        diag[r, a][0].wait_recv()
        sums[zs, kx, :, :cut] = sums[zs, kx, :, :cut] + left[zs]
        on_x[r, a].start()
        if len(diag[r, a]) > 1:
            diag[r, a][1].wait_recv()
            sums[zs, ky, :, cut:] = sums[zs, ky, :, cut:] + right[zs]
        on_y[r, a].start()

    def fourth(r, a):
        sums, _, _, _, gx, gy, gz = scratch[7 * a : 7 * a + 7]
        zs = zs_of[r]
        k = x * 2 + y
        on_x[r, a].wait_recv()
        on_y[r, a].wait_recv()
        if r:
            sums[zs, k] = (
                sums[zs, k].astype(F32) + gx[zs].astype(F32) + gy[zs].astype(F32)
            ).astype(sums.dtype)
            along[r, a].start()
        else:
            outs[a][...] = sums[zs, k].astype(F32) + gx[zs].astype(F32) + gy[zs].astype(F32)

    def last(a):
        gz = scratch[7 * a + 6]
        total = outs[a][...]
        for r in range(1, layers):
            along[r, a].wait_recv()
            total = total + gz[r].astype(F32)
        outs[a][...] = total

    def finish():
        for copy in copies.made:
            copy.wait_send()

    units = [(r, a) for r in order for a in count]
    return (
        [first]
        + [functools.partial(second, *u) for u in units]
        + [functools.partial(third, *u) for u in units]
        + [functools.partial(fourth, *u) for u in units]
        + [functools.partial(last, a) for a in count]
        + [finish]
    )


def scatter_kernel(layers, count, *refs):
    grads, outs, rest = refs[:count], refs[count : 2 * count], refs[2 * count :]
    greet(layers)
    for phase in scatter_phases(layers, grads, outs, rest[: 7 * count], *rest[7 * count :]):
        phase()


def scatter_all(layers, grads, ident, name):
    shapes = [g.shape[-2:] for g in grads]
    made = scatter_count(layers, shapes)
    return pl.pallas_call(
        functools.partial(scatter_kernel, layers, len(grads)),
        out_shape=[jax.ShapeDtypeStruct(s, F32) for s in shapes],
        in_specs=[pl.BlockSpec(memory_space=pl.ANY)] * len(grads),
        out_specs=[pl.BlockSpec(memory_space=pltpu.VMEM)] * len(grads),
        scratch_shapes=scatter_scratch(layers, shapes, [g.dtype for g in grads])
        + [
            pltpu.SemaphoreType.DMA((made,)),
            pltpu.SemaphoreType.DMA((made,)),
            pltpu.SemaphoreType.DMA((layers * len(grads),)),
        ],
        compiler_params=pltpu.CompilerParams(
            collective_id=ident, has_side_effects=True, vmem_limit_bytes=60 << 20
        ),
        name=name,
    )(*grads)


def norm_rows(v, gain, shift):
    mean = jnp.mean(v, axis=-1, keepdims=True)
    center = v - mean
    spread = jnp.mean(center * center, axis=-1, keepdims=True)
    return center * lax.rsqrt(spread + EPSILON) * gain + shift


def gelu_exact(v):
    return jax.nn.gelu(v, approximate=False)


def shards(
    mesh,
    tokens,
    cube_lengths,
    key_mask,
    cotangent,
    norm_gain,
    norm_shift,
    proj_weight,
    query_bias,
    value_bias,
    merge_weight,
    merge_bias,
    mlp_gain,
    mlp_shift,
    expand_weight,
    expand_bias,
    reduce_weight,
    reduce_bias,
):
    slots, local_len, width = tokens.shape
    full_len = key_mask.shape[1]
    seq = full_len // local_len
    half = seq // slots
    layers = mesh.shape["dp"] // 2
    devices = mesh.shape["dp"] * seq
    rows = slots * local_len
    me = lax.axis_index("seq")
    cube = me // half

    across = [(i, (i + half) % seq) for i in range(seq)]
    around = [
        [(g * half + i, g * half + (i + r) % half) for g in range(slots) for i in range(half)]
        for r in range(half)
    ]

    def swap(pair):
        own = lax.dynamic_index_in_dim(pair, cube, 0, keepdims=False)
        other = lax.dynamic_index_in_dim(pair, 1 - cube, 0, keepdims=False)
        return own, lax.ppermute(other, "seq", across)

    def swap_back(own, other):
        back = lax.ppermute(other, "seq", across).astype(own.dtype)
        first = jnp.where(cube == 0, own, back)
        second = jnp.where(cube == 0, back, own)
        return jnp.stack([first, second])

    vectors = (
        norm_gain,
        norm_shift,
        query_bias,
        value_bias,
        merge_bias,
        mlp_gain,
        mlp_shift,
        reduce_bias,
        expand_bias,
    )
    pad = 1024 - sum(v.shape[0] for v in vectors)
    vector_shard = jnp.pad(jnp.concatenate(vectors), (0, pad)).reshape(8, LANES)
    proj_full, packed_vectors, merge_full, expand_full, reduce_full = gather_all(
        layers, (proj_weight, vector_shard, merge_weight, expand_weight, reduce_weight), 0, "gather"
    )
    packed_vectors = packed_vectors.reshape(devices, 1024)
    proj_full = proj_full.reshape(width, -1)
    merge_full = merge_full.reshape(width, -1)
    expand_full = expand_full.reshape(width, -1)
    reduce_full = reduce_full.reshape(-1, width)
    wide = []
    start = 0
    for vector in vectors:
        size = vector.shape[0]
        wide.append(packed_vectors[:, start : start + size].reshape(-1).astype(F32))
        start += size
    (
        gain_first,
        shift_first,
        query_add,
        value_add,
        merge_add,
        gain_second,
        shift_second,
        reduce_add,
        expand_add,
    ) = wide
    own_tokens, other_tokens = swap(tokens)
    own_cot, other_cot = swap(cotangent)
    resid = jnp.concatenate([own_tokens, other_tokens]).astype(F32)
    upstream = jnp.concatenate([own_cot, other_cot])

    length = lax.dynamic_index_in_dim(cube_lengths, cube, 0, keepdims=False)
    mask = lax.dynamic_index_in_dim(key_mask, cube, 0, keepdims=False)
    bias_all = jnp.where((mask > 0) & (jnp.arange(full_len) < length), 0.0, -1e30).astype(F32)
    blocks = []
    for r in range(half):
        device = cube * half + (me + half - r) % half
        for index in (device, (device + half) % seq):
            blocks.append(lax.dynamic_slice_in_dim(bias_all, index * local_len, local_len))
    bias = jnp.concatenate(blocks)

    first_f, first_pull = jax.vjp(norm_rows, resid, gain_first, shift_first)
    first = first_f.astype(BF16)
    packed = jnp.dot(first, proj_full, preferred_element_type=F32)
    query = (packed[:, :width] + query_add).astype(BF16)
    query = query * jnp.asarray(HD**-0.5, BF16)
    keys = packed[:, width : 2 * width].astype(BF16)
    values = (packed[:, 2 * width :] + value_add).astype(BF16)
    keys_all = jnp.concatenate([keys] + [lax.ppermute(keys, "seq", a) for a in around[1:]])
    values_all = jnp.concatenate([values] + [lax.ppermute(values, "seq", a) for a in around[1:]])
    attn, lse = attn_fwd(query, keys_all, values_all, bias[None, :])

    middle = resid + jnp.dot(attn, merge_full, preferred_element_type=F32) + merge_add
    second_f, second_pull = jax.vjp(norm_rows, middle, gain_second, shift_second)
    second = second_f.astype(BF16)
    hidden = jnp.dot(second, expand_full, preferred_element_type=F32) + expand_add
    act_f, gelu_pull = jax.vjp(gelu_exact, hidden)
    act = act_f.astype(BF16)
    output = middle + jnp.dot(act, reduce_full, preferred_element_type=F32) + reduce_add
    output = output.astype(BF16)
    activations = swap_back(output[:local_len], output[local_len:])

    def pieces(grad):
        return grad.astype(BF16).reshape(layers, 4, 2, grad.shape[0] // devices, -1)

    upstream_f = upstream.astype(F32)
    reduce_bias_grad = jnp.sum(upstream_f, axis=0)
    reduce_weight_grad = pieces(
        jnp.einsum("rf,rd->fd", act, upstream, preferred_element_type=F32)
    )
    act_grad = jnp.einsum("rd,fd->rf", upstream, reduce_full, preferred_element_type=F32)
    hidden_grad = gelu_pull(act_grad)[0].astype(BF16)
    expand_bias_grad = jnp.sum(hidden_grad.astype(F32), axis=0)
    expand_weight_grad = pieces(
        jnp.einsum("rd,rf->df", second, hidden_grad, preferred_element_type=F32)
    )
    second_grad = jnp.einsum("rf,df->rd", hidden_grad, expand_full, preferred_element_type=F32)
    middle_norm, mlp_gain_grad, mlp_shift_grad = second_pull(second_grad)
    middle_grad = upstream_f + middle_norm
    merged_grad = middle_grad.astype(BF16)
    merge_bias_grad = jnp.sum(merged_grad.astype(F32), axis=0)
    merge_weight_grad = pieces(
        jnp.einsum("rd,re->de", attn, merged_grad, preferred_element_type=F32)
    )
    attn_grad = jnp.einsum("re,de->rd", merged_grad, merge_full, preferred_element_type=F32)
    attn_grad = attn_grad.astype(BF16)

    query_grad, key_parts, value_parts = attn_bwd(
        query, keys_all, values_all, attn_grad, attn, lse, bias[:, None]
    )

    def collect(parts):
        total = parts[:rows].astype(F32)
        for r in range(1, half):
            sent = parts[r * rows : (r + 1) * rows]
            back = [(j, i) for i, j in around[r]]
            total = total + lax.ppermute(sent, "seq", back).astype(F32)
        return total.astype(BF16)

    key_grad = collect(key_parts)
    value_grad = collect(value_parts)
    query_bias_grad = jnp.sum(query_grad.astype(F32), axis=0)
    value_bias_grad = jnp.sum(value_grad.astype(F32), axis=0)
    packed_grad = jnp.concatenate([query_grad, key_grad, value_grad], axis=1)
    proj_weight_grad = pieces(
        jnp.einsum("rd,re->de", first, packed_grad, preferred_element_type=F32)
    )
    first_grad = jnp.einsum("re,de->rd", packed_grad, proj_full, preferred_element_type=F32)
    resid_norm, norm_gain_grad, norm_shift_grad = first_pull(first_grad)
    input_sum = middle_grad + resid_norm
    input_grad = swap_back(input_sum[:local_len], input_sum[local_len:].astype(BF16))

    vector_grads = (
        norm_gain_grad,
        norm_shift_grad,
        query_bias_grad,
        value_bias_grad,
        merge_bias_grad,
        mlp_gain_grad,
        mlp_shift_grad,
        reduce_bias_grad,
        expand_bias_grad,
    )
    vector_grad = jnp.concatenate([g.reshape(devices, -1) for g in vector_grads], axis=1)
    vector_grad = jnp.pad(vector_grad, ((0, 0), (0, pad))).reshape(layers, 4, 2, 8, LANES)
    reduce_weight_grad, expand_weight_grad, merge_weight_grad, proj_weight_grad, summed = scatter_all(
        layers,
        (reduce_weight_grad, expand_weight_grad, merge_weight_grad, proj_weight_grad, vector_grad),
        1,
        "scatter",
    )
    summed = summed.reshape(-1)
    small = []
    start = 0
    for vector in vectors:
        size = vector.shape[0]
        small.append(summed[start : start + size])
        start += size
    (
        norm_gain_grad,
        norm_shift_grad,
        query_bias_grad,
        value_bias_grad,
        merge_bias_grad,
        mlp_gain_grad,
        mlp_shift_grad,
        reduce_bias_grad,
        expand_bias_grad,
    ) = small
    return (
        activations,
        input_grad,
        norm_gain_grad,
        norm_shift_grad,
        proj_weight_grad,
        query_bias_grad,
        value_bias_grad,
        merge_weight_grad,
        merge_bias_grad,
        mlp_gain_grad,
        mlp_shift_grad,
        expand_weight_grad,
        expand_bias_grad,
        reduce_weight_grad,
        reduce_bias_grad,
    )


def solution(mesh):
    whole, part = P(ALL, None), P(ALL)
    block = P("dp", "seq", None)
    in_specs = (
        block,
        P("dp"),
        P("dp", None),
        block,
        part,
        part,
        whole,
        part,
        part,
        whole,
        part,
        part,
        part,
        whole,
        part,
        whole,
        part,
    )
    out_specs = (
        block,
        block,
        part,
        part,
        whole,
        part,
        part,
        whole,
        part,
        part,
        part,
        whole,
        part,
        whole,
        part,
    )
    return jax.shard_map(
        functools.partial(shards, mesh), mesh=mesh, in_specs=in_specs, out_specs=out_specs, check_vma=False
    )
```

```python
import functools

import jax
import jax.numpy as jnp
from jax import lax
from jax.experimental import pallas as pl
from jax.experimental.pallas import tpu as pltpu
from jax.sharding import PartitionSpec as P

HD = 64
LANES = 128
EPSILON = 1e-06
F32 = jnp.float32
BF16 = jnp.bfloat16
ALL = ("dp", "seq")


MESH = pl.DeviceIdType.MESH


class Copies:
    def __init__(self, send, recv):
        self.send, self.recv, self.made = send, recv, []

    def make(self, src, dst, to):
        i = len(self.made)
        z, x, y, c = to
        copy = pltpu.make_async_remote_copy(
            src_ref=src,
            dst_ref=dst,
            send_sem=self.send.at[i],
            recv_sem=self.recv.at[i],
            device_id=(z * 2 + x, y * 2 + c),
            device_id_type=MESH,
        )
        self.made.append(copy)
        return copy


def place():
    dp, seq = lax.axis_index("dp"), lax.axis_index("seq")
    return dp // 2, dp % 2, seq // 2, seq % 2


def ring(layers):
    z, x, y, c = place()
    others = [((z + r) % layers, x, y, c) for r in range(1, layers)]
    return (z, x, y, 1 - c), (z, 1 - x, y, c), (z, x, 1 - y, c), others


def greet(layers):
    sibling, across_x, across_y, others = ring(layers)
    peers = [sibling, across_x, across_y] + others
    barrier = pltpu.get_barrier_semaphore()
    for z, x, y, c in peers:
        pl.semaphore_signal(
            barrier, inc=1, device_id=(z * 2 + x, y * 2 + c), device_id_type=MESH
        )
    pl.semaphore_wait(barrier, len(peers))


def cut_of(columns):
    return columns // 2 if columns % 256 == 0 else columns


KINDS = 10


def gather_phases(layers, shards, outs, send, recv, local):
    z, x, y, c = place()
    sibling, across_x, across_y, _ = ring(layers)
    above, below = ((z + 1) % layers, x, y, c), ((z + layers - 1) % layers, x, y, c)
    count = range(len(shards))

    def index(z, x, y, c):
        return ((z * 2 + x) * 2 + y) * 2 + c

    def copy(src, dst, a, kind, zs, to, sent=None):
        i = (a * KINDS + kind) * layers + zs
        j = (a * KINDS + (kind if sent is None else sent)) * layers + zs
        z, x, y, c = to
        return pltpu.make_async_remote_copy(
            src_ref=src,
            dst_ref=dst,
            send_sem=send.at[j],
            recv_sem=recv.at[i],
            device_id=(z * 2 + x, y * 2 + c),
            device_id_type=MESH,
        )

    mine = [
        pltpu.make_async_copy(shards[a], outs[a].at[index(z, x, y, c)], local.at[a]) for a in count
    ]
    sources = [(0, 0)]
    for d in range(1, layers):
        sources += [(1, d), (-1, d)]

    def unit(source, a):
        way, d = source
        zs = (z + layers - way * d) % layers
        there = None if d == 0 else (z >= d if way == 1 else z + d < layers)
        out = outs[a]
        here = out.at[index(zs, x, y, c)]
        src = shards[a] if d == 0 else here
        px = out.at[index(zs, 1 - x, y, c)]
        py = out.at[index(zs, x, 1 - y, c)]
        pd = out.at[index(zs, 1 - x, 1 - y, c)]
        columns = shards[a].shape[-1]
        cut = cut_of(columns)
        left = px if cut == columns else px.at[:, pl.ds(0, cut)]
        relay = [copy(left, left, a, 7, zs, across_y)]
        if cut < columns:
            right = py.at[:, pl.ds(cut, cut)]
            relay.append(copy(right, right, a, 8, zs, across_x))
        up = copy(src, here, a, 0, zs, above)
        down = copy(src, here, a, 0, zs, below, 9 if d == 0 else None)
        spread = [
            copy(src, here, a, 1, zs, across_x),
            copy(src, here, a, 2, zs, across_y),
            copy(src, here, a, 3, zs, sibling),
        ]
        sib = [copy(p, p, a, 4 + i, zs, sibling) for i, p in enumerate((px, py, pd))]
        return there, up, down, spread, relay, sib

    units = {(s, a): unit(s, a) for s in sources for a in count}

    def when(there, body):
        if there is None:
            body()
        else:
            pl.when(there)(body)

    def onward(source, up, down, act):
        way, d = source
        if way >= 0 and d < layers - 1:
            pl.when(z + 1 < layers)(lambda: act(up))
        if way <= 0 and d < layers - 1:
            pl.when(z > 0)(lambda: act(down))

    def second(source):
        for a in count:
            there, up, down, spread, relay, sib = units[source, a]

            def body():
                if source[1]:
                    up.wait_recv()
                else:
                    mine[a].start()
                onward(source, up, down, lambda copy: copy.start())
                for copy in spread:
                    copy.start()

            when(there, body)

    def third(source):
        for a in count:
            there, up, down, spread, relay, sib = units[source, a]

            def body():
                spread[0].wait_recv()
                relay[0].start()
                sib[0].start()
                spread[1].wait_recv()
                for copy in relay[1:]:
                    copy.start()
                sib[1].start()

            when(there, body)

    def fourth(source):
        for a in count:
            there, up, down, spread, relay, sib = units[source, a]

            def body():
                for copy in relay:
                    copy.wait_recv()
                sib[2].start()

            when(there, body)

    def last(source):
        for a in count:
            there, up, down, spread, relay, sib = units[source, a]

            def body():
                for copy in [spread[2]] + sib:
                    copy.wait_recv()
                onward(source, up, down, lambda copy: copy.wait_send())
                for copy in spread + relay + sib:
                    copy.wait_send()
                if source[1] == 0:
                    mine[a].wait()

            when(there, body)

    levels = []
    for d in range(layers + 2):
        level = []
        for lag, step in enumerate((second, third, fourth)):
            if lag <= d < layers + lag:
                level += [functools.partial(step, w) for w in sources if w[1] == d - lag]
        levels.append(level)
    return levels + [[functools.partial(last, w) for w in sources]]


def gather_kernel(layers, count, *refs):
    shards, outs = refs[:count], refs[count : 2 * count]
    greet(layers)
    for level in gather_phases(layers, shards, outs, *refs[2 * count :]):
        for phase in level:
            phase()


def gather_scratch(layers, count):
    return [
        pltpu.SemaphoreType.DMA((count * KINDS * layers,)),
        pltpu.SemaphoreType.DMA((count * KINDS * layers,)),
        pltpu.SemaphoreType.DMA((count,)),
    ]


def gather_all(layers, shards, ident, name):
    devices = layers * 8
    return pl.pallas_call(
        functools.partial(gather_kernel, layers, len(shards)),
        out_shape=[jax.ShapeDtypeStruct((devices,) + s.shape, s.dtype) for s in shards],
        in_specs=[pl.BlockSpec(memory_space=pltpu.VMEM)] * len(shards),
        out_specs=[pl.BlockSpec(memory_space=pl.ANY)] * len(shards),
        scratch_shapes=gather_scratch(layers, len(shards)),
        compiler_params=pltpu.CompilerParams(collective_id=ident, has_side_effects=True),
        name=name,
    )(*shards)


def scatter_scratch(layers, shapes, dtypes):
    made = []
    for (rows, columns), dtype in zip(shapes, dtypes):
        cut = cut_of(columns)
        made += [
            pltpu.VMEM((layers, 4, rows, columns), dtype),
            pltpu.VMEM((layers, 4, rows, columns), dtype),
            pltpu.VMEM((layers, rows, cut), dtype),
            pltpu.VMEM((layers, rows, cut), dtype),
            pltpu.VMEM((layers, rows, columns), dtype),
            pltpu.VMEM((layers, rows, columns), dtype),
            pltpu.VMEM((layers, rows, columns), dtype),
        ]
    return made


def scatter_count(layers, shapes):
    total = 0
    for _, columns in shapes:
        total += layers - 1 + layers * (4 if cut_of(columns) == columns else 5)
    return total


def scatter_phases(layers, grads, outs, scratch, send, recv, local):
    z, x, y, c = place()
    sibling, across_x, across_y, others = ring(layers)
    copies = Copies(send, recv)
    count = range(len(grads))
    kept, from_sib, diag, on_x, on_y, along, zs_of = {}, {}, {}, {}, {}, {}, {}
    order = list(range(1, layers)) + [0]
    for r in order:
        zs = (z + r) % layers
        zs_of[r] = zs
        for a in count:
            sums, terms, left, right, gx, gy, gz = scratch[7 * a : 7 * a + 7]
            columns = sums.shape[-1]
            cut = cut_of(columns)
            kept[r, a] = pltpu.make_async_copy(
                grads[a].at[zs, :, c], sums.at[zs], local.at[len(grads) * r + a]
            )
            from_sib[r, a] = copies.make(grads[a].at[zs, :, 1 - c], terms.at[zs], sibling)
            far = sums.at[zs, (1 - x) * 2 + 1 - y]
            if cut == columns:
                diag[r, a] = [copies.make(far, left.at[zs], across_y)]
            else:
                diag[r, a] = [
                    copies.make(far.at[:, pl.ds(0, cut)], left.at[zs], across_y),
                    copies.make(far.at[:, pl.ds(cut, cut)], right.at[zs], across_x),
                ]
            on_x[r, a] = copies.make(sums.at[zs, (1 - x) * 2 + y], gx.at[zs], across_x)
            on_y[r, a] = copies.make(sums.at[zs, x * 2 + 1 - y], gy.at[zs], across_y)
            if r:
                along[r, a] = copies.make(sums.at[zs, x * 2 + y], gz.at[r], others[r - 1])

    def first():
        for r in order:
            for a in count:
                kept[r, a].start()
                from_sib[r, a].start()

    def second(r, a):
        sums, terms = scratch[7 * a : 7 * a + 2]
        zs = zs_of[r]
        kept[r, a].wait()
        from_sib[r, a].wait_recv()
        for k in range(4):
            sums[zs, k] = sums[zs, k] + terms[zs, k]
        for copy in diag[r, a]:
            copy.start()

    def third(r, a):
        sums, _, left, right = scratch[7 * a : 7 * a + 4]
        zs = zs_of[r]
        cut = left.shape[-1]
        kx, ky = (1 - x) * 2 + y, x * 2 + 1 - y
        diag[r, a][0].wait_recv()
        sums[zs, kx, :, :cut] = sums[zs, kx, :, :cut] + left[zs]
        on_x[r, a].start()
        if len(diag[r, a]) > 1:
            diag[r, a][1].wait_recv()
            sums[zs, ky, :, cut:] = sums[zs, ky, :, cut:] + right[zs]
        on_y[r, a].start()

    def fourth(r, a):
        sums, _, _, _, gx, gy, gz = scratch[7 * a : 7 * a + 7]
        zs = zs_of[r]
        k = x * 2 + y
        on_x[r, a].wait_recv()
        on_y[r, a].wait_recv()
        if r:
            sums[zs, k] = (
                sums[zs, k].astype(F32) + gx[zs].astype(F32) + gy[zs].astype(F32)
            ).astype(sums.dtype)
            along[r, a].start()
        else:
            outs[a][...] = sums[zs, k].astype(F32) + gx[zs].astype(F32) + gy[zs].astype(F32)

    def last(a):
        gz = scratch[7 * a + 6]
        total = outs[a][...]
        for r in range(1, layers):
            along[r, a].wait_recv()
            total = total + gz[r].astype(F32)
        outs[a][...] = total

    def finish():
        for copy in copies.made:
            copy.wait_send()

    levels = [[first]]
    for i in range(layers + 2):
        level = []
        for lag, step in enumerate((second, third, fourth)):
            if lag <= i < layers + lag:
                level += [functools.partial(step, order[i - lag], a) for a in count]
        levels.append(level)
    return levels + [[functools.partial(last, a) for a in count] + [finish]]


def scatter_kernel(layers, count, *refs):
    grads, outs, rest = refs[:count], refs[count : 2 * count], refs[2 * count :]
    greet(layers)
    for level in scatter_phases(layers, grads, outs, rest[: 7 * count], *rest[7 * count :]):
        for phase in level:
            phase()


def scatter_all(layers, grads, ident, name):
    shapes = [g.shape[-2:] for g in grads]
    made = scatter_count(layers, shapes)
    return pl.pallas_call(
        functools.partial(scatter_kernel, layers, len(grads)),
        out_shape=[jax.ShapeDtypeStruct(s, F32) for s in shapes],
        in_specs=[pl.BlockSpec(memory_space=pl.ANY)] * len(grads),
        out_specs=[pl.BlockSpec(memory_space=pltpu.VMEM)] * len(grads),
        scratch_shapes=scatter_scratch(layers, shapes, [g.dtype for g in grads])
        + [
            pltpu.SemaphoreType.DMA((made,)),
            pltpu.SemaphoreType.DMA((made,)),
            pltpu.SemaphoreType.DMA((layers * len(grads),)),
        ],
        compiler_params=pltpu.CompilerParams(
            collective_id=ident, has_side_effects=True, vmem_limit_bytes=60 << 20
        ),
        name=name,
    )(*grads)


def head_lanes(rows, h):
    lane = lax.broadcasted_iota(jnp.int32, (rows, LANES), 1)
    return (lane < HD) if h == 0 else (lane >= HD)


def spread(phases, step, steps):
    late = []
    for at, group in phases:
        if at < steps:

            def body(group=group):
                for phase in group:
                    phase()

            pl.when(step == at)(body)
        else:
            late += group
    return late


def fwd_kernel(layers, pieces, count, *refs):
    q_ref, refs = refs[0], refs[1:]
    k_refs, v_refs, refs = refs[:pieces], refs[pieces : 2 * pieces], refs[2 * pieces :]
    bias_ref, shards, refs = refs[0], refs[1 : 1 + count], refs[1 + count :]
    o_ref, lse_ref, outs, sems = refs[0], refs[1], refs[2 : 2 + count], refs[2 + count :]
    step = pl.program_id(0) * pl.num_programs(1) + pl.program_id(1)
    levels = gather_phases(layers, shards, outs, *sems)

    @pl.when(step == 0)
    def _():
        greet(layers)

    late = spread([(5 * i, group) for i, group in enumerate(levels)], step, 18)

    tq = q_ref.shape[0]
    k = jnp.concatenate([r[...] for r in k_refs], axis=0)
    v = jnp.concatenate([r[...] for r in v_refs], axis=0)
    q = q_ref[...]
    results = []
    for h in range(2):
        qh = jnp.where(head_lanes(tq, h), q, jnp.zeros_like(q))
        s = lax.dot_general(qh, k, (((1,), (1,)), ((), ())), preferred_element_type=F32)
        s = s + bias_ref[...]
        top = jnp.max(s, axis=1, keepdims=True)
        e = jnp.exp(s - top)
        total = jnp.sum(e, axis=1, keepdims=True)
        results.append(jnp.dot(e.astype(BF16), v, preferred_element_type=F32) / total)
        lse = top + jnp.log(total)
        lse_ref[0, h : h + 1, :] = jnp.broadcast_to(lse, (tq, LANES)).T[0:1, :]
    o_ref[...] = jnp.where(head_lanes(tq, 0), results[0], results[1]).astype(BF16)

    @pl.when(step == pl.num_programs(0) * pl.num_programs(1) - 1)
    def _():
        for phase in late:
            phase()


def attn_fwd(layers, q, ks, vs, bias, shards, ident, tq=256):
    rows, width = q.shape
    keys = bias.shape[1]
    pairs = width // LANES
    row = pl.BlockSpec((tq, LANES), lambda p, i: (i, p))
    key = pl.BlockSpec((ks[0].shape[0], LANES), lambda p, i: (0, p))
    lse = pl.BlockSpec((1, 2, tq), lambda p, i: (p, 0, i))
    vmem, anywhere = pl.BlockSpec(memory_space=pltpu.VMEM), pl.BlockSpec(memory_space=pl.ANY)
    count = len(shards)
    return pl.pallas_call(
        functools.partial(fwd_kernel, layers, len(ks), count),
        grid=(pairs, rows // tq),
        in_specs=[row]
        + [key] * (2 * len(ks))
        + [pl.BlockSpec((1, keys), lambda p, i: (0, 0))]
        + [vmem] * count,
        out_specs=[row, lse] + [anywhere] * count,
        out_shape=[
            jax.ShapeDtypeStruct((rows, width), BF16),
            jax.ShapeDtypeStruct((pairs, 2, rows), F32),
        ]
        + [jax.ShapeDtypeStruct((layers * 8,) + s.shape, s.dtype) for s in shards],
        scratch_shapes=gather_scratch(layers, count),
        compiler_params=pltpu.CompilerParams(
            collective_id=ident, has_side_effects=True, vmem_limit_bytes=60 << 20
        ),
        name="attn_fwd",
    )(q, *ks, *vs, bias, *shards)


def bwd_kernel(layers, pieces, count, *refs):
    q_ref, refs = refs[0], refs[1:]
    k_refs, v_refs, refs = refs[:pieces], refs[pieces : 2 * pieces], refs[2 * pieces :]
    g_ref, o_ref, lse_ref, bias_ref, refs = refs[0], refs[1], refs[2], refs[3], refs[4:]
    grads, dq_ref, refs = refs[:count], refs[count], refs[count + 1 :]
    dk_refs, dv_refs, refs = refs[:pieces], refs[pieces : 2 * pieces], refs[2 * pieces :]
    outs, dk_acc, dv_acc, refs = refs[:count], refs[count], refs[count + 1], refs[count + 2 :]
    inner, last = pl.program_id(1), pl.num_programs(1) - 1
    step = pl.program_id(0) * pl.num_programs(1) + inner
    levels = scatter_phases(layers, grads, outs, refs[: 7 * count], *refs[7 * count :])

    @pl.when(step == 0)
    def _():
        greet(layers)

    late = spread([(max(0, 4 * i - 2), group) for i, group in enumerate(levels)], step, 18)

    @pl.when(inner == 0)
    def _():
        dk_acc[...] = jnp.zeros_like(dk_acc)
        dv_acc[...] = jnp.zeros_like(dv_acc)

    tq = q_ref.shape[0]
    k = jnp.concatenate([r[...] for r in k_refs], axis=0)
    v = jnp.concatenate([r[...] for r in v_refs], axis=0)
    q = q_ref[...]
    g = g_ref[...]
    go = g.astype(F32) * o_ref[...].astype(F32)
    dq = None
    for h in range(2):
        keep = head_lanes(tq, h)
        qh = jnp.where(keep, q, jnp.zeros_like(q))
        gh = jnp.where(keep, g, jnp.zeros_like(g))
        delta = jnp.sum(jnp.where(keep, go, 0.0), axis=1, keepdims=True)
        delta = jnp.broadcast_to(delta, (tq, LANES)).T[0:1, :]
        s = lax.dot_general(k, qh, (((1,), (1,)), ((), ())), preferred_element_type=F32)
        p = jnp.exp(s + bias_ref[...] - lse_ref[0, h : h + 1, :])
        dp = lax.dot_general(v, gh, (((1,), (1,)), ((), ())), preferred_element_type=F32)
        ds = (p * (dp - delta)).astype(BF16)
        dv_acc[...] += jnp.dot(p.astype(BF16), gh, preferred_element_type=F32)
        dk_acc[...] += jnp.dot(ds, qh, preferred_element_type=F32)
        kh = jnp.where(head_lanes(k.shape[0], h), k, jnp.zeros_like(k))
        part = lax.dot_general(ds, kh, (((0,), (0,)), ((), ())), preferred_element_type=F32)
        dq = part if dq is None else dq + part
    dq_ref[...] = (dq * HD**-0.5).astype(BF16)

    @pl.when(inner == last)
    def _():
        size = k_refs[0].shape[0]
        for j in range(pieces):
            dk_refs[j][...] = dk_acc[j * size : (j + 1) * size, :].astype(BF16)
            dv_refs[j][...] = dv_acc[j * size : (j + 1) * size, :].astype(BF16)

    @pl.when(step == pl.num_programs(0) * pl.num_programs(1) - 1)
    def _():
        for phase in late:
            phase()


def attn_bwd(layers, q, ks, vs, g, o, lse, bias, grads, ident, tq=256):
    rows, width = q.shape
    keys = bias.shape[0]
    pairs = width // LANES
    row = pl.BlockSpec((tq, LANES), lambda p, i: (i, p))
    key = pl.BlockSpec((ks[0].shape[0], LANES), lambda p, i: (0, p))
    stat = pl.BlockSpec((1, 2, tq), lambda p, i: (p, 0, i))
    vmem, anywhere = pl.BlockSpec(memory_space=pltpu.VMEM), pl.BlockSpec(memory_space=pl.ANY)
    count, pieces = len(grads), len(ks)
    shapes = [d.shape[-2:] for d in grads]
    made = scatter_count(layers, shapes)
    return pl.pallas_call(
        functools.partial(bwd_kernel, layers, pieces, count),
        grid=(pairs, rows // tq),
        in_specs=[row]
        + [key] * (2 * pieces)
        + [row, row, stat, pl.BlockSpec((keys, 1), lambda p, i: (0, 0))]
        + [anywhere] * count,
        out_specs=[row] + [key] * (2 * pieces) + [vmem] * count,
        out_shape=[jax.ShapeDtypeStruct((rows, width), BF16)]
        + [jax.ShapeDtypeStruct(k.shape, BF16) for k in ks + vs]
        + [jax.ShapeDtypeStruct(s, F32) for s in shapes],
        scratch_shapes=[pltpu.VMEM((keys, LANES), F32), pltpu.VMEM((keys, LANES), F32)]
        + scatter_scratch(layers, shapes, [d.dtype for d in grads])
        + [
            pltpu.SemaphoreType.DMA((made,)),
            pltpu.SemaphoreType.DMA((made,)),
            pltpu.SemaphoreType.DMA((layers * count,)),
        ],
        compiler_params=pltpu.CompilerParams(
            collective_id=ident, has_side_effects=True, vmem_limit_bytes=63 << 20
        ),
        name="attn_bwd",
    )(q, *ks, *vs, g, o, lse, bias, *grads)


def norm_rows(v, gain, shift):
    mean = jnp.mean(v, axis=-1, keepdims=True)
    center = v - mean
    spread = jnp.mean(center * center, axis=-1, keepdims=True)
    return center * lax.rsqrt(spread + EPSILON) * gain + shift


def gelu_exact(v):
    return jax.nn.gelu(v, approximate=False)


def shards(
    mesh,
    tokens,
    cube_lengths,
    key_mask,
    cotangent,
    norm_gain,
    norm_shift,
    proj_weight,
    query_bias,
    value_bias,
    merge_weight,
    merge_bias,
    mlp_gain,
    mlp_shift,
    expand_weight,
    expand_bias,
    reduce_weight,
    reduce_bias,
):
    slots, local_len, width = tokens.shape
    full_len = key_mask.shape[1]
    seq = full_len // local_len
    half = seq // slots
    layers = mesh.shape["dp"] // 2
    devices = mesh.shape["dp"] * seq
    me = lax.axis_index("seq")
    cube = me // half

    across = [(i, (i + half) % seq) for i in range(seq)]
    around = [
        [(g * half + i, g * half + (i + r) % half) for g in range(slots) for i in range(half)]
        for r in range(half)
    ]

    def swap(pair):
        own = lax.dynamic_index_in_dim(pair, cube, 0, keepdims=False)
        other = lax.dynamic_index_in_dim(pair, 1 - cube, 0, keepdims=False)
        return own, lax.ppermute(other, "seq", across)

    def swap_back(own, other):
        back = lax.ppermute(other, "seq", across).astype(own.dtype)
        first = jnp.where(cube == 0, own, back)
        second = jnp.where(cube == 0, back, own)
        return jnp.stack([first, second])

    vectors = (
        norm_gain,
        norm_shift,
        query_bias,
        value_bias,
        merge_bias,
        mlp_gain,
        mlp_shift,
        reduce_bias,
        expand_bias,
    )
    narrow = len(vectors) - 1
    total = sum(v.shape[0] for v in vectors)
    pad = 1024 - total
    vector_shard = jnp.pad(jnp.concatenate(vectors), (0, pad)).reshape(8, LANES)
    proj_full, vector_full = gather_all(layers, (proj_weight, vector_shard), 0, "gather")
    proj_full = proj_full.reshape(width, -1)
    vector_full = vector_full.reshape(devices, 1024)
    edge = narrow * (width // devices)
    table = vector_full[:, :edge].reshape(devices, narrow, -1).transpose(1, 0, 2)
    table = table.reshape(narrow, width).astype(F32)
    (
        gain_first,
        shift_first,
        query_add,
        value_add,
        merge_add,
        gain_second,
        shift_second,
        reduce_add,
    ) = [table[i] for i in range(narrow)]
    expand_add = vector_full[:, edge:total].reshape(-1).astype(F32)
    own_tokens, other_tokens = swap(tokens)
    own_cot, other_cot = swap(cotangent)
    resid = jnp.concatenate([own_tokens, other_tokens]).astype(F32)
    upstream = jnp.concatenate([own_cot, other_cot])

    length = lax.dynamic_index_in_dim(cube_lengths, cube, 0, keepdims=False)
    mask = lax.dynamic_index_in_dim(key_mask, cube, 0, keepdims=False)
    bias_all = jnp.where((mask > 0) & (jnp.arange(full_len) < length), 0.0, -1e30).astype(F32)
    blocks = []
    for r in range(half):
        device = cube * half + (me + half - r) % half
        for index in (device, (device + half) % seq):
            blocks.append(lax.dynamic_slice_in_dim(bias_all, index * local_len, local_len))
    bias = jnp.concatenate(blocks)

    first_f, first_pull = jax.vjp(norm_rows, resid, gain_first, shift_first)
    first = first_f.astype(BF16)
    packed = jnp.dot(first, proj_full, preferred_element_type=F32)
    query = (packed[:, :width] + query_add).astype(BF16)
    query = query * jnp.asarray(HD**-0.5, BF16)
    keys = packed[:, width : 2 * width].astype(BF16)
    values = (packed[:, 2 * width :] + value_add).astype(BF16)
    keys_all = [keys] + [lax.ppermute(keys, "seq", a) for a in around[1:]]
    values_all = [values] + [lax.ppermute(values, "seq", a) for a in around[1:]]
    attn, lse, merge_full, expand_full, reduce_full = attn_fwd(
        layers,
        query,
        keys_all,
        values_all,
        bias[None, :],
        (merge_weight, expand_weight, reduce_weight),
        1,
    )
    merge_full = merge_full.reshape(width, -1)
    expand_full = expand_full.reshape(width, -1)
    reduce_full = reduce_full.reshape(-1, width)

    middle = resid + jnp.dot(attn, merge_full, preferred_element_type=F32) + merge_add
    second_f, second_pull = jax.vjp(norm_rows, middle, gain_second, shift_second)
    second = second_f.astype(BF16)
    hidden = jnp.dot(second, expand_full, preferred_element_type=F32) + expand_add
    act_f, gelu_pull = jax.vjp(gelu_exact, hidden)
    act = act_f.astype(BF16)
    output = middle + jnp.dot(act, reduce_full, preferred_element_type=F32) + reduce_add
    output = output.astype(BF16)
    activations = swap_back(output[:local_len], output[local_len:])

    def pieces(grad):
        return grad.astype(BF16).reshape(layers, 4, 2, grad.shape[0] // devices, -1)

    upstream_f = upstream.astype(F32)
    reduce_bias_grad = jnp.sum(upstream_f, axis=0)
    reduce_weight_grad = pieces(
        jnp.einsum("rf,rd->fd", act, upstream, preferred_element_type=F32)
    )
    act_grad = jnp.einsum("rd,fd->rf", upstream, reduce_full, preferred_element_type=F32)
    hidden_grad = gelu_pull(act_grad)[0].astype(BF16)
    expand_bias_grad = jnp.sum(hidden_grad.astype(F32), axis=0)
    expand_weight_grad = pieces(
        jnp.einsum("rd,rf->df", second, hidden_grad, preferred_element_type=F32)
    )
    second_grad = jnp.einsum("rf,df->rd", hidden_grad, expand_full, preferred_element_type=F32)
    middle_norm, mlp_gain_grad, mlp_shift_grad = second_pull(second_grad)
    middle_grad = upstream_f + middle_norm
    merged_grad = middle_grad.astype(BF16)
    merge_bias_grad = jnp.sum(merged_grad.astype(F32), axis=0)
    merge_weight_grad = pieces(
        jnp.einsum("rd,re->de", attn, merged_grad, preferred_element_type=F32)
    )
    attn_grad = jnp.einsum("re,de->rd", merged_grad, merge_full, preferred_element_type=F32)
    attn_grad = attn_grad.astype(BF16)

    results = attn_bwd(
        layers,
        query,
        keys_all,
        values_all,
        attn_grad,
        attn,
        lse,
        bias[:, None],
        (reduce_weight_grad, expand_weight_grad, merge_weight_grad),
        2,
    )
    query_grad, key_parts, value_parts = (
        results[0],
        results[1 : 1 + half],
        results[1 + half : 1 + 2 * half],
    )
    reduce_weight_grad, expand_weight_grad, merge_weight_grad = results[1 + 2 * half :]

    def collect(parts):
        total = parts[0].astype(F32)
        for r in range(1, half):
            back = [(j, i) for i, j in around[r]]
            total = total + lax.ppermute(parts[r], "seq", back).astype(F32)
        return total.astype(BF16)

    key_grad = collect(key_parts)
    value_grad = collect(value_parts)
    query_bias_grad = jnp.sum(query_grad.astype(F32), axis=0)
    value_bias_grad = jnp.sum(value_grad.astype(F32), axis=0)
    packed_grad = jnp.concatenate([query_grad, key_grad, value_grad], axis=1)
    proj_weight_grad = pieces(
        jnp.einsum("rd,re->de", first, packed_grad, preferred_element_type=F32)
    )
    first_grad = jnp.einsum("re,de->rd", packed_grad, proj_full, preferred_element_type=F32)
    resid_norm, norm_gain_grad, norm_shift_grad = first_pull(first_grad)
    input_sum = middle_grad + resid_norm
    input_grad = swap_back(input_sum[:local_len], input_sum[local_len:].astype(BF16))

    vector_grads = (
        norm_gain_grad,
        norm_shift_grad,
        query_bias_grad,
        value_bias_grad,
        merge_bias_grad,
        mlp_gain_grad,
        mlp_shift_grad,
        reduce_bias_grad,
        expand_bias_grad,
    )
    vector_grad = jnp.stack(vector_grads[:narrow]).reshape(narrow, devices, -1).transpose(1, 0, 2)
    vector_grad = jnp.concatenate(
        [vector_grad.reshape(devices, -1), vector_grads[narrow].reshape(devices, -1)], axis=1
    )
    vector_grad = jnp.pad(vector_grad, ((0, 0), (0, pad))).reshape(layers, 4, 2, 8, LANES)
    proj_weight_grad, summed = scatter_all(layers, (proj_weight_grad, vector_grad), 3, "scatter")
    summed = summed.reshape(-1)
    small = []
    start = 0
    for vector in vectors:
        size = vector.shape[0]
        small.append(summed[start : start + size])
        start += size
    (
        norm_gain_grad,
        norm_shift_grad,
        query_bias_grad,
        value_bias_grad,
        merge_bias_grad,
        mlp_gain_grad,
        mlp_shift_grad,
        reduce_bias_grad,
        expand_bias_grad,
    ) = small
    return (
        activations,
        input_grad,
        norm_gain_grad,
        norm_shift_grad,
        proj_weight_grad,
        query_bias_grad,
        value_bias_grad,
        merge_weight_grad,
        merge_bias_grad,
        mlp_gain_grad,
        mlp_shift_grad,
        expand_weight_grad,
        expand_bias_grad,
        reduce_weight_grad,
        reduce_bias_grad,
    )


def solution(mesh):
    whole, part = P(ALL, None), P(ALL)
    block = P("dp", "seq", None)
    in_specs = (
        block,
        P("dp"),
        P("dp", None),
        block,
        part,
        part,
        whole,
        part,
        part,
        whole,
        part,
        part,
        part,
        whole,
        part,
        whole,
        part,
    )
    out_specs = (
        block,
        block,
        part,
        part,
        whole,
        part,
        part,
        whole,
        part,
        part,
        part,
        whole,
        part,
        whole,
        part,
    )
    return jax.shard_map(
        functools.partial(shards, mesh), mesh=mesh, in_specs=in_specs, out_specs=out_specs, check_vma=False
    )
```
